32 devices in a mesh: row: 4 (over y, x), col: 4 (over z), crop: 2 (over core).
Axes of the slice: x: 2, y: 2, z: 4, core: 2. Of those that a mesh axis runs over, the one named last changes fastest.
Arguments:
- pair_repr: bfloat16 [256, 128, 128], P(('crop', 'row'), 'col'), parts along dimension 0, may hold values from -6 to 6
- pair_mask: int32 [256, 128], P(('crop', 'row'), 'col'), parts along dimension 0, may hold values 0 or 1
- out_left_w: bfloat16 [128, 256], replicated, may hold values from -0.5 to 0.5
- out_right_w: bfloat16 [128, 256], replicated, may hold values from -0.5 to 0.5
- out_gate_w: bfloat16 [128, 128], replicated, may hold values from -0.5 to 0.5
- out_final_w: bfloat16 [128, 128], replicated, may hold values from -0.5 to 0.5
- in_left_w: bfloat16 [128, 256], replicated, may hold values from -0.5 to 0.5
- in_right_w: bfloat16 [128, 256], replicated, may hold values from -0.5 to 0.5
- in_gate_w: bfloat16 [128, 128], replicated, may hold values from -0.5 to 0.5
- in_final_w: bfloat16 [128, 128], replicated, may hold values from -0.5 to 0.5
- trans_in_w: bfloat16 [128, 1024], replicated, may hold values from -0.5 to 0.5
- trans_out_w: bfloat16 [512, 128], replicated, may hold values from -0.25 to 0.25
Outputs:
- pair_out: bfloat16 [256, 128, 128], P(('crop', 'row'), 'col'), parts along dimension 0
The draws below stay inside these ranges and needn't reach their ends.
There are 2 independent parts, one for each index of `crop`. The reference program is written for one: setup_inputs(seed, part) draws one part's arguments, and reference() takes and returns one part's arrays. A program takes and returns all parts, laid end to end along the dimension named above; an argument that names none is the same for every part. Nothing has to cross between parts.
All inputs are finite; a program needn't handle non-finite values. No bound on the sum of `pair_mask` on one device may be relied on, other than what follows from the above.
Results may differ from the reference program's by a relative error of at most 0.015.
Values may be sent and summed in bfloat16 or wider, within the bound.
No kernel may reach another device: no remote copies, remote signals or barrier semaphores. Data moves between devices by JAX's collectives and lax.ppermute only.
A program may use at most 128 MiB of HBM per device.

```python
import jax
import jax.numpy as jnp
from jax import lax

C = 128
H = 128
F = 512
N = 128


def place_ends(array, rng, smallest, high):
    longest = array.shape.index(max(array.shape))
    spots = []
    for shift in (0, 1):
        where = [jax.random.randint(jax.random.fold_in(rng, axis), (), 0, length) for axis, length in enumerate(array.shape)]
        where[longest] = (where[longest] + shift) % array.shape[longest]
        spots.append(tuple(where))
    return array.at[spots[0]].set(smallest).at[spots[1]].set(high)


def steps_of(key, dims, split, low, top_value):
    factor_of, own = 1.0, jax.random.fold_in(key, 6)
    for dim, shards_of in split:
        heights = jnp.exp(jax.random.uniform(jax.random.fold_in(own, dim), (shards_of,), jnp.float32, low / len(split), top_value / len(split)))
        factor_of = factor_of * jnp.repeat(heights, dims[dim] // shards_of).reshape([-1 if axis == dim else 1 for axis in range(len(dims))])
    return factor_of


def centred(stream_key, extent, scale, reach, shards=(), kind=jnp.bfloat16):
    entries = jax.random.normal(stream_key, extent, jnp.float32) * scale
    if len(shards) > 0:
        entries = steps_of(stream_key, extent, shards, -0.22, 0.18) * entries
    return jnp.clip(entries, min=-reach, max=reach).astype(kind)


def setup_inputs(seed: int = 0, part: int = 0) -> dict:
    key_of = jax.random.split(jax.random.key(seed), 13)
    own_keys = jax.random.split(jax.random.fold_in(key_of[12], part), 13)
    return {
        "pair_repr": centred(own_keys[0], (N, N, C), 1.0, 6.0, ((0, 4), (1, 4))),
        "pair_mask": place_ends((jax.random.randint(own_keys[1], (N, N), 0, 8) < 7).astype(jnp.int32), jax.random.fold_in(own_keys[1], 1), 0, 1),
        "out_left_w": centred(key_of[2], (C, 2 * H), C ** -0.5, 0.5),
        "out_right_w": centred(key_of[3], (C, 2 * H), C ** -0.5, 0.5),
        "out_gate_w": centred(key_of[4], (C, C), C ** -0.5, 0.5),
        "out_final_w": centred(key_of[5], (H, C), H ** -0.5, 0.5),
        "in_left_w": centred(key_of[6], (C, 2 * H), C ** -0.5, 0.5),
        "in_right_w": centred(key_of[7], (C, 2 * H), C ** -0.5, 0.5),
        "in_gate_w": centred(key_of[8], (C, C), C ** -0.5, 0.5),
        "in_final_w": centred(key_of[9], (H, C), H ** -0.5, 0.5),
        "trans_in_w": centred(key_of[10], (C, 2 * F), C ** -0.5, 0.5),
        "trans_out_w": centred(key_of[11], (F, C), F ** -0.5, 0.25),
    }


epsilon = 1e-05

def layer_norm(values):
    average = lax.optimization_barrier(jnp.mean(values, axis=-1, keepdims=True))
    centered = values - average
    spread = lax.optimization_barrier(jnp.mean(centered * centered, axis=-1, keepdims=True))
    return centered * lax.rsqrt(spread + epsilon)

def gated(normed, weight, mask_vals):
    projected = jnp.dot(normed, weight, preferred_element_type=jnp.float32)
    half_width = weight.shape[1] // 2
    result = jax.nn.sigmoid(projected[..., :half_width]) * projected[..., half_width:]
    return (result * mask_vals[..., None]).astype(jnp.bfloat16)

def triangle_update(pair_repr, mask_vals, left_w, right_w, gate_w, final_w, formula):
    normed = layer_norm(pair_repr.astype(jnp.float32)).astype(jnp.bfloat16)
    left_vals = gated(normed, left_w, mask_vals)
    right_vals = gated(normed, right_w, mask_vals)
    gate_vals = jax.nn.sigmoid(jnp.dot(normed, gate_w, preferred_element_type=jnp.float32))
    triangle = jnp.einsum(formula, left_vals.astype(jnp.float32), right_vals.astype(jnp.float32))
    tri_norm = layer_norm(triangle).astype(jnp.bfloat16)
    update = jnp.dot(tri_norm, final_w, preferred_element_type=jnp.float32)
    return (pair_repr.astype(jnp.float32) + gate_vals * update).astype(jnp.bfloat16)

def reference(pair_repr, pair_mask, out_left_w, out_right_w, out_gate_w, out_final_w, in_left_w, in_right_w, in_gate_w, in_final_w, trans_in_w, trans_out_w):
    mask_vals = pair_mask.astype(jnp.float32)
    middle = triangle_update(pair_repr, mask_vals, out_left_w, out_right_w, out_gate_w, out_final_w, 'ikh,jkh->ijh')
    after_in = triangle_update(middle, mask_vals, in_left_w, in_right_w, in_gate_w, in_final_w, 'kih,kjh->ijh')

    def transition_row(row_vals):
        normed = layer_norm(row_vals.astype(jnp.float32)).astype(jnp.bfloat16)
        projected = jnp.dot(normed, trans_in_w, preferred_element_type=jnp.float32)
        half_width = trans_in_w.shape[1] // 2
        hidden = (jax.nn.silu(projected[..., :half_width]) * projected[..., half_width:]).astype(jnp.bfloat16)
        result = row_vals.astype(jnp.float32) + jnp.dot(hidden, trans_out_w, preferred_element_type=jnp.float32)
        return result.astype(jnp.bfloat16)
    return lax.map(transition_row, after_in)
```

```python
import functools

import jax
import jax.numpy as jnp
from jax import lax
from jax.experimental import pallas as pl
from jax.experimental.pallas import tpu as pltpu
from jax.sharding import PartitionSpec as P

epsilon = 1e-05
LANES = 128
SUB = 8
F32, BF16 = jnp.float32, jnp.bfloat16


def norm_rows(values):
    average = jnp.mean(values, axis=0, keepdims=True)
    centered = values - average
    spread = jnp.mean(centered * centered, axis=0, keepdims=True)
    return (centered * lax.rsqrt(spread + epsilon)).astype(BF16)


def sigmoid(values):
    return 0.5 * jnp.tanh(0.5 * values) + 0.5


def dot(a, b):
    return jnp.dot(a, b, preferred_element_type=F32)


def swap_groups(values, width):
    values = list(values)
    count = len(values)
    group = lax.broadcasted_iota(jnp.int32, values[0].shape, 1) // width
    bit = count // 2
    while bit:
        low = (group & bit) == 0
        for at in range(count):
            if at & bit:
                continue
            one, two = values[at], values[at | bit]
            values[at] = jnp.where(low, one, pltpu.roll(two, bit * width, 1))
            values[at | bit] = jnp.where(low, pltpu.roll(one, LANES - bit * width, 1), two)
        bit //= 2
    return values


def lane_mask(mask_ref, lane_ref, groups):
    rows, width = mask_ref.shape
    count = rows // groups
    for lo in range(groups):
        lane_ref[:, lo * width : (lo + 1) * width] = mask_ref[lo * count : (lo + 1) * count, :].astype(F32)


def project(normed, step, per, left_w, right_w, gate_w, lane_ref, scr_ref, gate_ref):
    half = left_w.shape[0] // 2
    high = lane_ref.shape[0]
    for side, weight in enumerate((left_w, right_w)):
        both = dot(weight, normed)
        value = sigmoid(both[:half]) * both[half:]
        for u in range(per):
            hi = step * per + u
            piece = value[:, u * LANES : (u + 1) * LANES] * lane_ref[hi : hi + 1, :]
            scr_ref[side, pl.ds(hi, half, stride=high), :] = piece
    gate_ref[:, step * per * LANES : (step + 1) * per * LANES] = sigmoid(dot(gate_w, normed))


def flush(scr_ref, send_ref):
    parts = send_ref.shape[0]
    for side in range(2):
        send_ref[:, side] = scr_ref[side].reshape(parts, -1, LANES).astype(BF16)


def finish(step, per, tri_ref, gate_ref, base_ref, final_w):
    high = tri_ref.shape[0] // final_w.shape[1]
    rows = final_w.shape[1]
    triangle = jnp.concatenate(
        [tri_ref[pl.ds(step * per + u, rows, stride=high), :] for u in range(per)], axis=1
    )
    update = dot(final_w, norm_rows(triangle))
    span = slice(step * per * LANES, (step + 1) * per * LANES)
    return base_ref[:, span].astype(F32) + gate_ref[:, span] * update


def open_kernel(per, groups, x_ref, mask_ref, lw_ref, rw_ref, gw_ref, send_ref, gate_ref, base_ref, lane_ref, scr_ref):
    rows, width, channels = x_ref.shape
    high = rows // groups
    lane_mask(mask_ref, lane_ref, groups)
    left_w, right_w, gate_w = lw_ref[...].T, rw_ref[...].T, gw_ref[...].T
    for step in range(high // per):
        tokens = [x_ref[lo * high + step * per + u] for u in range(per) for lo in range(groups)]
        values = jnp.concatenate([t.astype(F32) for t in tokens], axis=0).T
        base_ref[:, step * per * LANES : (step + 1) * per * LANES] = values.astype(BF16)
        project(norm_rows(values), step, per, left_w, right_w, gate_w, lane_ref, scr_ref, gate_ref)
    flush(scr_ref, send_ref)


def middle_kernel(per, groups, back_ref, gate0_ref, base0_ref, fw_ref, mask_ref, lw_ref, rw_ref, gw_ref,
                  send_ref, gate_ref, base_ref, lane_ref, scr_ref, tri_ref):
    lane_mask(mask_ref, lane_ref, groups)
    tri_ref[...] = back_ref[...].reshape(tri_ref.shape).astype(F32)
    final_w = fw_ref[...].T
    left_w, right_w, gate_w = lw_ref[...].T, rw_ref[...].T, gw_ref[...].T
    for step in range(lane_ref.shape[0] // per):
        middle = finish(step, per, tri_ref, gate0_ref, base0_ref, final_w).astype(BF16)
        base_ref[:, step * per * LANES : (step + 1) * per * LANES] = middle
        project(norm_rows(middle.astype(F32)), step, per, left_w, right_w, gate_w, lane_ref, scr_ref, gate_ref)
    flush(scr_ref, send_ref)


def close_kernel(per, groups, back_ref, gate_ref, base_ref, fw_ref, inw_ref, outw_ref, out_ref, tri_ref):
    rows, width, channels = out_ref.shape
    high = rows // groups
    tri_ref[...] = back_ref[...].reshape(tri_ref.shape).astype(F32)
    final_w, in_w, out_w = fw_ref[...].T, inw_ref[...].T, outw_ref[...].T
    half = in_w.shape[0] // 2
    for step in range(high // per):
        after = finish(step, per, tri_ref, gate_ref, base_ref, final_w).astype(BF16).astype(F32)
        both = dot(in_w, norm_rows(after))
        swish = both[:half]
        hidden = (swish * sigmoid(swish) * both[half:]).astype(BF16)
        result = (after + dot(out_w, hidden)).T
        for u in range(per):
            for lo in range(groups):
                at = (u * groups + lo) * width
                out_ref[lo * high + step * per + u] = result[at : at + width].astype(BF16)


def triangle_kernel(side, groups, incoming, got_ref, send_ref):
    parts, _, rows, _ = got_ref.shape
    width = LANES // groups
    mine = rows // SUB
    turned = []
    for which in range(2):
        per_row = []
        for r in range(side):
            blocks = [got_ref[r * side + c, which].astype(F32) for c in range(side)]
            per_row.append(swap_groups(blocks, width))
        turned.append(per_row)
    sums = []
    for h in range(mine):
        span = slice(h * SUB, (h + 1) * SUB)
        left = jnp.concatenate([turned[0][r][lo][span] for lo in range(groups) for r in range(side)], axis=0).astype(BF16)
        if incoming:
            right = jnp.concatenate([turned[1][r][lo][span] for lo in range(groups) for r in range(side)], axis=0).astype(BF16)
            total = lax.dot_general(left, right, (((0,), (0,)), ((), ())), preferred_element_type=F32)
            pick = lambda r, lo: (r * groups + lo) * SUB
        else:
            right = jnp.concatenate([turned[1][r][lo][span] for r in range(side) for lo in range(groups)], axis=0).astype(BF16)
            total = lax.dot_general(left, right, (((1,), (1,)), ((), ())), preferred_element_type=F32)
            pick = lambda r, lo: (lo * side + r) * SUB
        sums.append([[total[pick(r, lo) : pick(r, lo) + SUB] for lo in range(groups)] for r in range(side)])
    for r in range(side):
        blocks = [jnp.concatenate([sums[h][r][lo] for h in range(mine)], axis=0) for lo in range(groups)]
        for c, block in enumerate(swap_groups(blocks, width)):
            send_ref[r * side + c] = block.astype(BF16)


def channel_split(side, *args):
    (x, mask, out_left_w, out_right_w, out_gate_w, out_final_w, in_left_w, in_right_w, in_gate_w, in_final_w,
     trans_in_w, trans_out_w) = args
    axes = ("row", "col")
    rows, width, channels = x.shape
    hidden = out_final_w.shape[0]
    groups = LANES // width
    high = rows // groups
    parts = side * side
    tokens = rows * width
    block = hidden // parts * high
    per = 2
    shape = jax.ShapeDtypeStruct
    send = shape((parts, 2, block, LANES), BF16)
    back = shape((parts, block, LANES), BF16)
    gate = shape((channels, tokens), F32)
    base = shape((channels, tokens), BF16)
    lane_scr = pltpu.VMEM((high, LANES), F32)
    scr = pltpu.VMEM((2, hidden * high, LANES), F32)
    tri_scr = pltpu.VMEM((hidden * high, LANES), F32)

    def exchange(values):
        return lax.all_to_all(values, axes, split_axis=0, concat_axis=0, tiled=True)

    def triangle(got, incoming, name):
        return pl.pallas_call(functools.partial(triangle_kernel, side, groups, incoming), out_shape=back, name=name)(got)

    sent, gate_out, base_out = pl.pallas_call(
        functools.partial(open_kernel, per, groups), out_shape=(send, gate, base), scratch_shapes=[lane_scr, scr], name="open"
    )(x, mask, out_left_w, out_right_w, out_gate_w)
    returned = exchange(triangle(exchange(sent), False, "outgoing"))
    sent, gate_in, base_in = pl.pallas_call(
        functools.partial(middle_kernel, per, groups), out_shape=(send, gate, base),
        scratch_shapes=[lane_scr, scr, tri_scr], name="middle",
    )(returned, gate_out, base_out, out_final_w, mask, in_left_w, in_right_w, in_gate_w)
    returned = exchange(triangle(exchange(sent), True, "incoming"))
    return pl.pallas_call(
        functools.partial(close_kernel, per, groups), out_shape=shape(x.shape, BF16), scratch_shapes=[tri_scr], name="close"
    )(returned, gate_in, base_in, in_final_w, trans_in_w, trans_out_w)


def layer_norm(values):
    average = jnp.mean(values, axis=-1, keepdims=True)
    centered = values - average
    spread = jnp.mean(centered * centered, axis=-1, keepdims=True)
    return centered * lax.rsqrt(spread + epsilon)


def gated(normed, weight, mask_vals):
    projected = jnp.dot(normed, weight, preferred_element_type=F32)
    half_width = weight.shape[1] // 2
    result = jax.nn.sigmoid(projected[..., :half_width]) * projected[..., half_width:]
    result = result * mask_vals[..., None]
    return result.astype(BF16)


def finish_plain(pair_repr, normed, triangle, gate_w, final_w):
    gate_vals = jax.nn.sigmoid(jnp.dot(normed, gate_w, preferred_element_type=F32))
    tri_norm = layer_norm(triangle).astype(BF16)
    update = jnp.dot(tri_norm, final_w, preferred_element_type=F32)
    return (pair_repr.astype(F32) + gate_vals * update).astype(BF16)


def gathers(pair_repr, pair_mask, out_left_w, out_right_w, out_gate_w, out_final_w, in_left_w, in_right_w, in_gate_w,
            in_final_w, trans_in_w, trans_out_w):
    mask_vals = pair_mask.astype(F32)
    normed_out = layer_norm(pair_repr.astype(F32)).astype(BF16)
    outbound = gated(normed_out, out_right_w, mask_vals)
    turned_right = lax.all_to_all(
        lax.all_to_all(outbound, "row", split_axis=0, concat_axis=0, tiled=True),
        "col", split_axis=0, concat_axis=1, tiled=True,
    )
    left_tile = gated(normed_out, out_left_w, mask_vals)
    gathered = lax.all_gather(left_tile, "col", axis=1, tiled=True)
    triangle = jnp.einsum(
        "ikh,jkh->ijh", gathered, lax.all_gather(turned_right, "row", axis=0, tiled=True), preferred_element_type=F32
    )
    middle = finish_plain(pair_repr, normed_out, triangle, out_gate_w, out_final_w)
    normed_in = layer_norm(middle.astype(F32)).astype(BF16)
    outbound_left = gated(normed_in, in_left_w, mask_vals)
    turned_left = lax.all_to_all(
        lax.all_to_all(outbound_left, "col", split_axis=1, concat_axis=1, tiled=True),
        "row", split_axis=1, concat_axis=0, tiled=True,
    )
    right_tile = gated(normed_in, in_right_w, mask_vals)
    column_panel = lax.all_gather(right_tile, "row", axis=0, tiled=True)
    triangle_in = jnp.einsum(
        "kih,kjh->ijh", lax.all_gather(turned_left, "col", axis=1, tiled=True), column_panel, preferred_element_type=F32
    )
    after_in = finish_plain(middle, normed_in, triangle_in, in_gate_w, in_final_w)
    normed_mix = layer_norm(after_in.astype(F32)).astype(BF16)
    projected = jnp.dot(normed_mix, trans_in_w, preferred_element_type=F32)
    half_width = trans_in_w.shape[1] // 2
    hidden = (jax.nn.silu(projected[..., :half_width]) * projected[..., half_width:]).astype(BF16)
    result = after_in.astype(F32) + jnp.dot(hidden, trans_out_w, preferred_element_type=F32)
    return result.astype(BF16)


def shards(row_size, col_size, *args):
    rows, width, channels = args[0].shape
    hidden = args[5].shape[0]
    fits = (
        row_size == col_size
        and rows == width
        and row_size * rows == LANES
        and rows % (LANES // width) == 0
        and rows // (LANES // width) == SUB
        and hidden % (row_size * col_size) == 0
        and channels == LANES
        and hidden == LANES
    )
    if fits:
        return channel_split(row_size, *args)
    return gathers(*args)


def solution(mesh):
    tile = P(("crop", "row"), "col")
    in_specs = (P(("crop", "row"), "col", None), tile) + (P(),) * 10
    out_specs = P(("crop", "row"), "col", None)
    body = functools.partial(shards, mesh.shape["row"], mesh.shape["col"])
    return jax.shard_map(body, mesh=mesh, in_specs=in_specs, out_specs=out_specs, check_vma=False)
```

```python
import functools

import jax
import jax.numpy as jnp
from jax import lax
from jax.experimental import pallas as pl
from jax.experimental.pallas import tpu as pltpu
from jax.sharding import PartitionSpec as P

epsilon = 1e-05
LANES = 128
SUB = 8
F32, BF16 = jnp.float32, jnp.bfloat16
PARAMS = pltpu.CompilerParams(vmem_limit_bytes=16 * 1024 * 1024)


def norm_rows(values):
    average = jnp.mean(values, axis=0, keepdims=True)
    centered = values - average
    spread = jnp.mean(centered * centered, axis=0, keepdims=True)
    return (centered * lax.rsqrt(spread + epsilon)).astype(BF16)


def sigmoid(values):
    return 0.5 * jnp.tanh(0.5 * values) + 0.5


def dot(a, b):
    return jnp.dot(a, b, preferred_element_type=F32)


def swap_groups(values, width):
    values = list(values)
    count = len(values)
    group = lax.broadcasted_iota(jnp.int32, values[0].shape, 1) // width
    bit = count // 2
    while bit:
        low = (group & bit) == 0
        for at in range(count):
            if at & bit:
                continue
            one, two = values[at], values[at | bit]
            values[at] = jnp.where(low, one, pltpu.roll(two, bit * width, 1))
            values[at | bit] = jnp.where(low, pltpu.roll(one, LANES - bit * width, 1), two)
        bit //= 2
    return values


def lane_mask(mask_ref, lane_ref, groups):
    rows, width = mask_ref.shape
    count = rows // groups
    for lo in range(groups):
        lane_ref[:, lo * width : (lo + 1) * width] = mask_ref[lo * count : (lo + 1) * count, :].astype(F32)


def project(normed, step, per, left_w, right_w, gate_w, lane_ref, scr_ref, gate_ref):
    half = left_w.shape[0] // 2
    high = lane_ref.shape[0]
    for side, weight in enumerate((left_w, right_w)):
        both = dot(weight, normed)
        value = sigmoid(both[:half]) * both[half:]
        for u in range(per):
            hi = step * per + u
            piece = value[:, u * LANES : (u + 1) * LANES] * lane_ref[hi : hi + 1, :]
            scr_ref[side, pl.ds(hi, half, stride=high), :] = piece
    gate_ref[:, step * per * LANES : (step + 1) * per * LANES] = sigmoid(dot(gate_w, normed))


def flush(scr_ref, send_ref):
    parts = send_ref.shape[0]
    for side in range(2):
        send_ref[:, side] = scr_ref[side].reshape(parts, -1, LANES).astype(BF16)


def finish(step, per, tri_ref, gate_ref, base_ref, final_w):
    high = tri_ref.shape[0] // final_w.shape[1]
    rows = final_w.shape[1]
    triangle = jnp.concatenate(
        [tri_ref[pl.ds(step * per + u, rows, stride=high), :] for u in range(per)], axis=1
    )
    update = dot(final_w, norm_rows(triangle))
    span = slice(step * per * LANES, (step + 1) * per * LANES)
    return base_ref[:, span].astype(F32) + gate_ref[:, span] * update


def open_kernel(per, groups, x_ref, mask_ref, lw_ref, rw_ref, gw_ref, send_ref, gate_ref, base_ref, lane_ref, scr_ref):
    rows, width, channels = x_ref.shape
    high = rows // groups
    lane_mask(mask_ref, lane_ref, groups)
    left_w, right_w, gate_w = lw_ref[...].T, rw_ref[...].T, gw_ref[...].T
    for step in range(high // per):
        tokens = [x_ref[lo * high + step * per + u] for u in range(per) for lo in range(groups)]
        values = jnp.concatenate([t.astype(F32) for t in tokens], axis=0).T
        base_ref[:, step * per * LANES : (step + 1) * per * LANES] = values.astype(BF16)
        project(norm_rows(values), step, per, left_w, right_w, gate_w, lane_ref, scr_ref, gate_ref)
    flush(scr_ref, send_ref)


def middle_kernel(per, groups, back_ref, gate0_ref, base0_ref, fw_ref, mask_ref, lw_ref, rw_ref, gw_ref,
                  send_ref, gate_ref, base_ref, lane_ref, scr_ref, tri_ref):
    lane_mask(mask_ref, lane_ref, groups)
    tri_ref[...] = back_ref[...].reshape(tri_ref.shape).astype(F32)
    final_w = fw_ref[...].T
    left_w, right_w, gate_w = lw_ref[...].T, rw_ref[...].T, gw_ref[...].T
    for step in range(lane_ref.shape[0] // per):
        middle = finish(step, per, tri_ref, gate0_ref, base0_ref, final_w).astype(BF16)
        base_ref[:, step * per * LANES : (step + 1) * per * LANES] = middle
        project(norm_rows(middle.astype(F32)), step, per, left_w, right_w, gate_w, lane_ref, scr_ref, gate_ref)
    flush(scr_ref, send_ref)


def close_kernel(per, groups, back_ref, gate_ref, base_ref, fw_ref, inw_ref, outw_ref, out_ref, tri_ref):
    rows, width, channels = out_ref.shape
    high = rows // groups
    tri_ref[...] = back_ref[...].reshape(tri_ref.shape).astype(F32)
    final_w, in_w, out_w = fw_ref[...].T, inw_ref[...].T, outw_ref[...].T
    half = in_w.shape[0] // 2
    for step in range(high // per):
        after = finish(step, per, tri_ref, gate_ref, base_ref, final_w).astype(BF16).astype(F32)
        both = dot(in_w, norm_rows(after))
        swish = both[:half]
        hidden = (swish * sigmoid(swish) * both[half:]).astype(BF16)
        result = (after + dot(out_w, hidden)).T
        for u in range(per):
            for lo in range(groups):
                at = (u * groups + lo) * width
                out_ref[lo * high + step * per + u] = result[at : at + width].astype(BF16)


def triangle_kernel(side, groups, incoming, got_ref, send_ref):
    parts, _, rows, _ = got_ref.shape
    width = LANES // groups
    mine = rows // SUB
    turned = []
    for which in range(2):
        per_row = []
        for r in range(side):
            blocks = [got_ref[r * side + c, which].astype(F32) for c in range(side)]
            per_row.append(swap_groups(blocks, width))
        turned.append(per_row)
    sums = []
    for h in range(mine):
        span = slice(h * SUB, (h + 1) * SUB)
        left = jnp.concatenate([turned[0][r][lo][span] for lo in range(groups) for r in range(side)], axis=0).astype(BF16)
        if incoming:
            right = jnp.concatenate([turned[1][r][lo][span] for lo in range(groups) for r in range(side)], axis=0).astype(BF16)
            total = lax.dot_general(left, right, (((0,), (0,)), ((), ())), preferred_element_type=F32)
            pick = lambda r, lo: (r * groups + lo) * SUB
        else:
            right = jnp.concatenate([turned[1][r][lo][span] for r in range(side) for lo in range(groups)], axis=0).astype(BF16)
            total = lax.dot_general(left, right, (((1,), (1,)), ((), ())), preferred_element_type=F32)
            pick = lambda r, lo: (lo * side + r) * SUB
        sums.append([[total[pick(r, lo) : pick(r, lo) + SUB] for lo in range(groups)] for r in range(side)])
    for r in range(side):
        blocks = [jnp.concatenate([sums[h][r][lo] for h in range(mine)], axis=0) for lo in range(groups)]
        for c, block in enumerate(swap_groups(blocks, width)):
            send_ref[r * side + c] = block.astype(BF16)


def channel_split(side, *args):
    (x, mask, out_left_w, out_right_w, out_gate_w, out_final_w, in_left_w, in_right_w, in_gate_w, in_final_w,
     trans_in_w, trans_out_w) = args
    axes = ("row", "col")
    rows, width, channels = x.shape
    hidden = out_final_w.shape[0]
    groups = LANES // width
    high = rows // groups
    parts = side * side
    tokens = rows * width
    block = hidden // parts * high
    per = 2
    shape = jax.ShapeDtypeStruct
    send = shape((parts, 2, block, LANES), BF16)
    back = shape((parts, block, LANES), BF16)
    gate = shape((channels, tokens), F32)
    base = shape((channels, tokens), BF16)
    lane_scr = pltpu.VMEM((high, LANES), F32)
    scr = pltpu.VMEM((2, hidden * high, LANES), F32)
    tri_scr = pltpu.VMEM((hidden * high, LANES), F32)

    def exchange(values):
        return lax.all_to_all(values, axes, split_axis=0, concat_axis=0, tiled=True)

    def triangle(got, incoming, name):
        return pl.pallas_call(functools.partial(triangle_kernel, side, groups, incoming), out_shape=back, name=name, compiler_params=PARAMS)(got)

    sent, gate_out, base_out = pl.pallas_call(
        functools.partial(open_kernel, per, groups), out_shape=(send, gate, base), scratch_shapes=[lane_scr, scr], name="open", compiler_params=PARAMS
    )(x, mask, out_left_w, out_right_w, out_gate_w)
    returned = exchange(triangle(exchange(sent), False, "outgoing"))
    sent, gate_in, base_in = pl.pallas_call(
        functools.partial(middle_kernel, per, groups), out_shape=(send, gate, base),
        scratch_shapes=[lane_scr, scr, tri_scr], name="middle", compiler_params=PARAMS,
    )(returned, gate_out, base_out, out_final_w, mask, in_left_w, in_right_w, in_gate_w)
    returned = exchange(triangle(exchange(sent), True, "incoming"))
    return pl.pallas_call(
        functools.partial(close_kernel, per, groups), out_shape=shape(x.shape, BF16), scratch_shapes=[tri_scr], name="close", compiler_params=PARAMS
    )(returned, gate_in, base_in, in_final_w, trans_in_w, trans_out_w)


def layer_norm(values):
    average = jnp.mean(values, axis=-1, keepdims=True)
    centered = values - average
    spread = jnp.mean(centered * centered, axis=-1, keepdims=True)
    return centered * lax.rsqrt(spread + epsilon)


def gated(normed, weight, mask_vals):
    projected = jnp.dot(normed, weight, preferred_element_type=F32)
    half_width = weight.shape[1] // 2
    result = jax.nn.sigmoid(projected[..., :half_width]) * projected[..., half_width:]
    result = result * mask_vals[..., None]
    return result.astype(BF16)


def finish_plain(pair_repr, normed, triangle, gate_w, final_w):
    gate_vals = jax.nn.sigmoid(jnp.dot(normed, gate_w, preferred_element_type=F32))
    tri_norm = layer_norm(triangle).astype(BF16)
    update = jnp.dot(tri_norm, final_w, preferred_element_type=F32)
    return (pair_repr.astype(F32) + gate_vals * update).astype(BF16)


def gathers(pair_repr, pair_mask, out_left_w, out_right_w, out_gate_w, out_final_w, in_left_w, in_right_w, in_gate_w,
            in_final_w, trans_in_w, trans_out_w):
    mask_vals = pair_mask.astype(F32)
    normed_out = layer_norm(pair_repr.astype(F32)).astype(BF16)
    outbound = gated(normed_out, out_right_w, mask_vals)
    turned_right = lax.all_to_all(
        lax.all_to_all(outbound, "row", split_axis=0, concat_axis=0, tiled=True),
        "col", split_axis=0, concat_axis=1, tiled=True,
    )
    left_tile = gated(normed_out, out_left_w, mask_vals)
    gathered = lax.all_gather(left_tile, "col", axis=1, tiled=True)
    triangle = jnp.einsum(
        "ikh,jkh->ijh", gathered, lax.all_gather(turned_right, "row", axis=0, tiled=True), preferred_element_type=F32
    )
    middle = finish_plain(pair_repr, normed_out, triangle, out_gate_w, out_final_w)
    normed_in = layer_norm(middle.astype(F32)).astype(BF16)
    outbound_left = gated(normed_in, in_left_w, mask_vals)
    turned_left = lax.all_to_all(
        lax.all_to_all(outbound_left, "col", split_axis=1, concat_axis=1, tiled=True),
        "row", split_axis=1, concat_axis=0, tiled=True,
    )
    right_tile = gated(normed_in, in_right_w, mask_vals)
    column_panel = lax.all_gather(right_tile, "row", axis=0, tiled=True)
    triangle_in = jnp.einsum(
        "kih,kjh->ijh", lax.all_gather(turned_left, "col", axis=1, tiled=True), column_panel, preferred_element_type=F32
    )
    after_in = finish_plain(middle, normed_in, triangle_in, in_gate_w, in_final_w)
    normed_mix = layer_norm(after_in.astype(F32)).astype(BF16)
    projected = jnp.dot(normed_mix, trans_in_w, preferred_element_type=F32)
    half_width = trans_in_w.shape[1] // 2
    hidden = (jax.nn.silu(projected[..., :half_width]) * projected[..., half_width:]).astype(BF16)
    result = after_in.astype(F32) + jnp.dot(hidden, trans_out_w, preferred_element_type=F32)
    return result.astype(BF16)


def shards(row_size, col_size, *args):
    rows, width, channels = args[0].shape
    hidden = args[5].shape[0]
    fits = (
        row_size == col_size
        and rows == width
        and row_size * rows == LANES
        and rows % (LANES // width) == 0
        and rows // (LANES // width) == SUB
        and hidden % (row_size * col_size) == 0
        and channels == LANES
        and hidden == LANES
    )
    if fits:
        return channel_split(row_size, *args)
    return gathers(*args)


def solution(mesh):
    tile = P(("crop", "row"), "col")
    in_specs = (P(("crop", "row"), "col", None), tile) + (P(),) * 10
    out_specs = P(("crop", "row"), "col", None)
    body = functools.partial(shards, mesh.shape["row"], mesh.shape["col"])
    return jax.shard_map(body, mesh=mesh, in_specs=in_specs, out_specs=out_specs, check_vma=False)
```

```python
import functools

import jax
import jax.numpy as jnp
from jax import lax
from jax.experimental import pallas as pl
from jax.experimental.pallas import tpu as pltpu
from jax.sharding import PartitionSpec as P

epsilon = 1e-05
LANES = 128
SUB = 8
F32, BF16 = jnp.float32, jnp.bfloat16
OFFSET = 5000
PARAMS = pltpu.CompilerParams(vmem_limit_bytes=16 * 1024 * 1024)


def norm_rows(values):
    average = jnp.mean(values, axis=0, keepdims=True)
    centered = values - average
    spread = jnp.mean(centered * centered, axis=0, keepdims=True)
    return (centered * lax.rsqrt(spread + epsilon)).astype(BF16)


def sigmoid(values):
    return 0.5 * jnp.tanh(0.5 * values) + 0.5


def dot(a, b):
    return jnp.dot(a, b, preferred_element_type=F32)


def swap_groups(values, width):
    values = list(values)
    count = len(values)
    group = lax.broadcasted_iota(jnp.int32, values[0].shape, 1) // width
    bit = count // 2
    while bit:
        low = (group & bit) == 0
        for at in range(count):
            if at & bit:
                continue
            one, two = values[at], values[at | bit]
            values[at] = jnp.where(low, one, pltpu.roll(two, bit * width, 1))
            values[at | bit] = jnp.where(low, pltpu.roll(one, LANES - bit * width, 1), two)
        bit //= 2
    return values


def lane_mask(mask_ref, lane_ref, groups):
    rows, width = mask_ref.shape
    count = rows // groups
    for lo in range(groups):
        lane_ref[:, lo * width : (lo + 1) * width] = mask_ref[lo * count : (lo + 1) * count, :].astype(F32)


def project(normed, step, per, left_w, right_w, gate_w, lane_ref, scr_ref, gate_ref):
    half = left_w.shape[0] // 2
    high = lane_ref.shape[0]
    for side, weight in enumerate((left_w, right_w)):
        both = dot(weight, normed)
        value = sigmoid(both[:half]) * both[half:]
        for u in range(per):
            hi = step * per + u
            piece = value[:, u * LANES : (u + 1) * LANES] * lane_ref[hi : hi + 1, :]
            scr_ref[side, pl.ds(hi, half, stride=high), :] = piece
    gate_ref[:, step * per * LANES : (step + 1) * per * LANES] = sigmoid(dot(gate_w, normed))


def flush(scr_ref, send_ref):
    parts = send_ref.shape[0]
    for side in range(2):
        send_ref[:, side] = scr_ref[side].reshape(parts, -1, LANES).astype(BF16)


def finish(step, per, tri_ref, gate_ref, base_ref, final_w):
    high = tri_ref.shape[0] // final_w.shape[1]
    rows = final_w.shape[1]
    triangle = jnp.concatenate(
        [tri_ref[pl.ds(step * per + u, rows, stride=high), :] for u in range(per)], axis=1
    )
    update = dot(final_w, norm_rows(triangle))
    span = slice(step * per * LANES, (step + 1) * per * LANES)
    return base_ref[:, span].astype(F32) + gate_ref[:, span] * update


def open_kernel(per, groups, *refs):
    count = 5
    far, refs = refs[:count], refs[count:]
    send_ref, gate_ref, base_ref, lane_ref, scr_ref, *near, sems = refs
    copies = [pltpu.make_async_copy(a, b, sems.at[at]) for at, (a, b) in enumerate(zip(far, near))]
    for copy in copies:
        copy.start()
    x_ref, mask_ref, lw_ref, rw_ref, gw_ref = near
    rows, width, channels = x_ref.shape
    high = rows // groups

    @pl.when(lax.axis_index("crop") == 0)
    def _():
        pl.delay(OFFSET)

    for copy in copies:
        copy.wait()
    lane_mask(mask_ref, lane_ref, groups)
    left_w, right_w, gate_w = lw_ref[...].T, rw_ref[...].T, gw_ref[...].T
    for step in range(high // per):
        tokens = [x_ref[lo * high + step * per + u] for u in range(per) for lo in range(groups)]
        values = jnp.concatenate([t.astype(F32) for t in tokens], axis=0).T
        base_ref[:, step * per * LANES : (step + 1) * per * LANES] = values.astype(BF16)
        project(norm_rows(values), step, per, left_w, right_w, gate_w, lane_ref, scr_ref, gate_ref)
    flush(scr_ref, send_ref)


def middle_kernel(per, groups, back_ref, gate0_ref, base0_ref, fw_ref, mask_ref, lw_ref, rw_ref, gw_ref,
                  send_ref, gate_ref, base_ref, lane_ref, scr_ref, tri_ref):
    lane_mask(mask_ref, lane_ref, groups)
    tri_ref[...] = back_ref[...].reshape(tri_ref.shape).astype(F32)
    final_w = fw_ref[...].T
    left_w, right_w, gate_w = lw_ref[...].T, rw_ref[...].T, gw_ref[...].T
    for step in range(lane_ref.shape[0] // per):
        middle = finish(step, per, tri_ref, gate0_ref, base0_ref, final_w).astype(BF16)
        base_ref[:, step * per * LANES : (step + 1) * per * LANES] = middle
        project(norm_rows(middle.astype(F32)), step, per, left_w, right_w, gate_w, lane_ref, scr_ref, gate_ref)
    flush(scr_ref, send_ref)


def close_kernel(per, groups, back_ref, gate_ref, base_ref, fw_ref, inw_ref, outw_ref, out_ref, tri_ref):
    rows, width, channels = out_ref.shape
    high = rows // groups
    tri_ref[...] = back_ref[...].reshape(tri_ref.shape).astype(F32)
    final_w, in_w, out_w = fw_ref[...].T, inw_ref[...].T, outw_ref[...].T
    half = in_w.shape[0] // 2
    for step in range(high // per):
        after = finish(step, per, tri_ref, gate_ref, base_ref, final_w).astype(BF16).astype(F32)
        both = dot(in_w, norm_rows(after))
        swish = both[:half]
        hidden = (swish * sigmoid(swish) * both[half:]).astype(BF16)
        result = (after + dot(out_w, hidden)).T
        for u in range(per):
            for lo in range(groups):
                at = (u * groups + lo) * width
                out_ref[lo * high + step * per + u] = result[at : at + width].astype(BF16)


def triangle_kernel(side, groups, incoming, got_ref, send_ref):
    parts, _, rows, _ = got_ref.shape
    width = LANES // groups
    mine = rows // SUB
    turned = []
    for which in range(2):
        per_row = []
        for r in range(side):
            blocks = [got_ref[r * side + c, which].astype(F32) for c in range(side)]
            per_row.append(swap_groups(blocks, width))
        turned.append(per_row)
    sums = []
    for h in range(mine):
        span = slice(h * SUB, (h + 1) * SUB)
        left = jnp.concatenate([turned[0][r][lo][span] for lo in range(groups) for r in range(side)], axis=0).astype(BF16)
        if incoming:
            right = jnp.concatenate([turned[1][r][lo][span] for lo in range(groups) for r in range(side)], axis=0).astype(BF16)
            total = lax.dot_general(left, right, (((0,), (0,)), ((), ())), preferred_element_type=F32)
            pick = lambda r, lo: (r * groups + lo) * SUB
        else:
            right = jnp.concatenate([turned[1][r][lo][span] for r in range(side) for lo in range(groups)], axis=0).astype(BF16)
            total = lax.dot_general(left, right, (((1,), (1,)), ((), ())), preferred_element_type=F32)
            pick = lambda r, lo: (lo * side + r) * SUB
        sums.append([[total[pick(r, lo) : pick(r, lo) + SUB] for lo in range(groups)] for r in range(side)])
    for r in range(side):
        blocks = [jnp.concatenate([sums[h][r][lo] for h in range(mine)], axis=0) for lo in range(groups)]
        for c, block in enumerate(swap_groups(blocks, width)):
            send_ref[r * side + c] = block.astype(BF16)


def channel_split(side, *args):
    (x, mask, out_left_w, out_right_w, out_gate_w, out_final_w, in_left_w, in_right_w, in_gate_w, in_final_w,
     trans_in_w, trans_out_w) = args
    axes = ("row", "col")
    rows, width, channels = x.shape
    hidden = out_final_w.shape[0]
    groups = LANES // width
    high = rows // groups
    parts = side * side
    tokens = rows * width
    block = hidden // parts * high
    per = 2
    shape = jax.ShapeDtypeStruct
    send = shape((parts, 2, block, LANES), BF16)
    back = shape((parts, block, LANES), BF16)
    gate = shape((channels, tokens), F32)
    base = shape((channels, tokens), BF16)
    lane_scr = pltpu.VMEM((high, LANES), F32)
    scr = pltpu.VMEM((2, hidden * high, LANES), F32)
    tri_scr = pltpu.VMEM((hidden * high, LANES), F32)

    def exchange(values):
        return lax.all_to_all(values, axes, split_axis=0, concat_axis=0, tiled=True)

    def triangle(got, incoming, name):
        return pl.pallas_call(functools.partial(triangle_kernel, side, groups, incoming), out_shape=back, name=name, compiler_params=PARAMS)(got)

    first = (x, mask, out_left_w, out_right_w, out_gate_w)
    sent, gate_out, base_out = pl.pallas_call(
        functools.partial(open_kernel, per, groups), out_shape=(send, gate, base), name="open", compiler_params=pltpu.CompilerParams(vmem_limit_bytes=60 * 1024 * 1024),
        in_specs=[pl.BlockSpec(memory_space=pltpu.HBM)] * len(first),
        scratch_shapes=[lane_scr, scr] + [pltpu.VMEM(a.shape, a.dtype) for a in first] + [pltpu.SemaphoreType.DMA((len(first),))],
    )(*first)
    returned = exchange(triangle(exchange(sent), False, "outgoing"))
    sent, gate_in, base_in = pl.pallas_call(
        functools.partial(middle_kernel, per, groups), out_shape=(send, gate, base),
        scratch_shapes=[lane_scr, scr, tri_scr], name="middle", compiler_params=PARAMS,
    )(returned, gate_out, base_out, out_final_w, mask, in_left_w, in_right_w, in_gate_w)
    returned = exchange(triangle(exchange(sent), True, "incoming"))
    return pl.pallas_call(
        functools.partial(close_kernel, per, groups), out_shape=shape(x.shape, BF16), scratch_shapes=[tri_scr], name="close", compiler_params=PARAMS
    )(returned, gate_in, base_in, in_final_w, trans_in_w, trans_out_w)


def layer_norm(values):
    average = jnp.mean(values, axis=-1, keepdims=True)
    centered = values - average
    spread = jnp.mean(centered * centered, axis=-1, keepdims=True)
    return centered * lax.rsqrt(spread + epsilon)


def gated(normed, weight, mask_vals):
    projected = jnp.dot(normed, weight, preferred_element_type=F32)
    half_width = weight.shape[1] // 2
    result = jax.nn.sigmoid(projected[..., :half_width]) * projected[..., half_width:]
    result = result * mask_vals[..., None]
    return result.astype(BF16)


def finish_plain(pair_repr, normed, triangle, gate_w, final_w):
    gate_vals = jax.nn.sigmoid(jnp.dot(normed, gate_w, preferred_element_type=F32))
    tri_norm = layer_norm(triangle).astype(BF16)
    update = jnp.dot(tri_norm, final_w, preferred_element_type=F32)
    return (pair_repr.astype(F32) + gate_vals * update).astype(BF16)


def gathers(pair_repr, pair_mask, out_left_w, out_right_w, out_gate_w, out_final_w, in_left_w, in_right_w, in_gate_w,
            in_final_w, trans_in_w, trans_out_w):
    mask_vals = pair_mask.astype(F32)
    normed_out = layer_norm(pair_repr.astype(F32)).astype(BF16)
    outbound = gated(normed_out, out_right_w, mask_vals)
    turned_right = lax.all_to_all(
        lax.all_to_all(outbound, "row", split_axis=0, concat_axis=0, tiled=True),
        "col", split_axis=0, concat_axis=1, tiled=True,
    )
    left_tile = gated(normed_out, out_left_w, mask_vals)
    gathered = lax.all_gather(left_tile, "col", axis=1, tiled=True)
    triangle = jnp.einsum(
        "ikh,jkh->ijh", gathered, lax.all_gather(turned_right, "row", axis=0, tiled=True), preferred_element_type=F32
    )
    middle = finish_plain(pair_repr, normed_out, triangle, out_gate_w, out_final_w)
    normed_in = layer_norm(middle.astype(F32)).astype(BF16)
    outbound_left = gated(normed_in, in_left_w, mask_vals)
    turned_left = lax.all_to_all(
        lax.all_to_all(outbound_left, "col", split_axis=1, concat_axis=1, tiled=True),
        "row", split_axis=1, concat_axis=0, tiled=True,
    )
    right_tile = gated(normed_in, in_right_w, mask_vals)
    column_panel = lax.all_gather(right_tile, "row", axis=0, tiled=True)
    triangle_in = jnp.einsum(
        "kih,kjh->ijh", lax.all_gather(turned_left, "col", axis=1, tiled=True), column_panel, preferred_element_type=F32
    )
    after_in = finish_plain(middle, normed_in, triangle_in, in_gate_w, in_final_w)
    normed_mix = layer_norm(after_in.astype(F32)).astype(BF16)
    projected = jnp.dot(normed_mix, trans_in_w, preferred_element_type=F32)
    half_width = trans_in_w.shape[1] // 2
    hidden = (jax.nn.silu(projected[..., :half_width]) * projected[..., half_width:]).astype(BF16)
    result = after_in.astype(F32) + jnp.dot(hidden, trans_out_w, preferred_element_type=F32)
    return result.astype(BF16)


def shards(row_size, col_size, *args):
    rows, width, channels = args[0].shape
    hidden = args[5].shape[0]
    fits = (
        row_size == col_size
        and rows == width
        and row_size * rows == LANES
        and rows % (LANES // width) == 0
        and rows // (LANES // width) == SUB
        and hidden % (row_size * col_size) == 0
        and channels == LANES
        and hidden == LANES
    )
    if fits:
        return channel_split(row_size, *args)
    return gathers(*args)


def solution(mesh):
    tile = P(("crop", "row"), "col")
    in_specs = (P(("crop", "row"), "col", None), tile) + (P(),) * 10
    out_specs = P(("crop", "row"), "col", None)
    body = functools.partial(shards, mesh.shape["row"], mesh.shape["col"])
    return jax.shard_map(body, mesh=mesh, in_specs=in_specs, out_specs=out_specs, check_vma=False)
```

```python
import functools

import jax
import jax.numpy as jnp
from jax import lax
from jax.experimental import pallas as pl
from jax.experimental.pallas import tpu as pltpu
from jax.sharding import PartitionSpec as P

epsilon = 1e-05
LANES = 128
SUB = 8
F32, BF16 = jnp.float32, jnp.bfloat16
OFFSET = 5000
PARAMS = pltpu.CompilerParams(vmem_limit_bytes=16 * 1024 * 1024)


def norm_rows(values):
    average = jnp.mean(values, axis=0, keepdims=True)
    centered = values - average
    spread = jnp.mean(centered * centered, axis=0, keepdims=True)
    return (centered * lax.rsqrt(spread + epsilon)).astype(BF16)


def sigmoid(values):
    return 0.5 * jnp.tanh(0.5 * values) + 0.5


def dot(a, b):
    return jnp.dot(a, b, preferred_element_type=F32)


def swap_groups(values, width):
    values = list(values)
    count = len(values)
    group = lax.broadcasted_iota(jnp.int32, values[0].shape, 1) // width
    bit = count // 2
    while bit:
        low = (group & bit) == 0
        for at in range(count):
            if at & bit:
                continue
            one, two = values[at], values[at | bit]
            values[at] = jnp.where(low, one, pltpu.roll(two, bit * width, 1))
            values[at | bit] = jnp.where(low, pltpu.roll(one, LANES - bit * width, 1), two)
        bit //= 2
    return values


def lane_mask(mask_ref, lane_ref, groups):
    rows, width = mask_ref.shape
    count = rows // groups
    for lo in range(groups):
        lane_ref[:, lo * width : (lo + 1) * width] = mask_ref[lo * count : (lo + 1) * count, :].astype(F32)


def project(normed, step, per, left_w, right_w, gate_w, lane_ref, scr_ref, gate_ref):
    half = left_w.shape[0] // 2
    high = lane_ref.shape[0]
    for side, weight in enumerate((left_w, right_w)):
        both = dot(weight, normed)
        value = sigmoid(both[:half]) * both[half:]
        for u in range(per):
            hi = step * per + u
            piece = value[:, u * LANES : (u + 1) * LANES] * lane_ref[hi : hi + 1, :]
            scr_ref[side, pl.ds(hi, half, stride=high), :] = piece
    gate_ref[:, step * per * LANES : (step + 1) * per * LANES] = sigmoid(dot(gate_w, normed))


def flush(scr_ref, send_ref):
    parts = send_ref.shape[0]
    for side in range(2):
        send_ref[:, side] = scr_ref[side].reshape(parts, -1, LANES).astype(BF16)


def finish(step, per, tri_ref, gate_ref, base_ref, final_w):
    high = tri_ref.shape[0] // final_w.shape[1]
    rows = final_w.shape[1]
    triangle = jnp.concatenate(
        [tri_ref[pl.ds(step * per + u, rows, stride=high), :] for u in range(per)], axis=1
    )
    update = dot(final_w, norm_rows(triangle))
    span = slice(step * per * LANES, (step + 1) * per * LANES)
    return base_ref[:, span].astype(F32) + gate_ref[:, span] * update


def open_kernel(per, groups, *refs):
    count = 5
    far, refs = refs[:count], refs[count:]
    send_ref, gate_ref, base_ref, lane_ref, scr_ref, *near, sems = refs
    copies = [pltpu.make_async_copy(a, b, sems.at[at]) for at, (a, b) in enumerate(zip(far, near))]
    for copy in copies:
        copy.start()
    x_ref, mask_ref, lw_ref, rw_ref, gw_ref = near
    rows, width, channels = x_ref.shape
    high = rows // groups

    @pl.when(lax.axis_index("crop") == 0)
    def _():
        pl.delay(OFFSET)

    for copy in copies:
        copy.wait()
    lane_mask(mask_ref, lane_ref, groups)
    left_w, right_w, gate_w = lw_ref[...].T, rw_ref[...].T, gw_ref[...].T
    for step in range(high // per):
        tokens = [x_ref[lo * high + step * per + u] for u in range(per) for lo in range(groups)]
        values = jnp.concatenate([t.astype(F32) for t in tokens], axis=0).T
        base_ref[:, step * per * LANES : (step + 1) * per * LANES] = values.astype(BF16)
        project(norm_rows(values), step, per, left_w, right_w, gate_w, lane_ref, scr_ref, gate_ref)
    flush(scr_ref, send_ref)


def middle_kernel(per, groups, back_ref, gate0_ref, base0_ref, fw_ref, mask_ref, lw_ref, rw_ref, gw_ref,
                  send_ref, gate_ref, base_ref, lane_ref, scr_ref, tri_ref):
    lane_mask(mask_ref, lane_ref, groups)
    tri_ref[...] = back_ref[...].reshape(tri_ref.shape).astype(F32)
    final_w = fw_ref[...].T
    left_w, right_w, gate_w = lw_ref[...].T, rw_ref[...].T, gw_ref[...].T
    for step in range(lane_ref.shape[0] // per):
        middle = finish(step, per, tri_ref, gate0_ref, base0_ref, final_w).astype(BF16)
        base_ref[:, step * per * LANES : (step + 1) * per * LANES] = middle
        project(norm_rows(middle.astype(F32)), step, per, left_w, right_w, gate_w, lane_ref, scr_ref, gate_ref)
    flush(scr_ref, send_ref)


def close_kernel(per, groups, back_ref, gate_ref, base_ref, fw_ref, inw_ref, outw_ref, out_ref, tri_ref):
    rows, width, channels = out_ref.shape
    high = rows // groups
    tri_ref[...] = back_ref[...].reshape(tri_ref.shape).astype(F32)
    final_w, in_w, out_w = fw_ref[...].T, inw_ref[...].T, outw_ref[...].T
    half = in_w.shape[0] // 2
    for step in range(high // per):
        after = finish(step, per, tri_ref, gate_ref, base_ref, final_w).astype(BF16).astype(F32)
        both = dot(in_w, norm_rows(after))
        swish = both[:half]
        hidden = (swish * sigmoid(swish) * both[half:]).astype(BF16)
        result = (after + dot(out_w, hidden)).T
        for u in range(per):
            for lo in range(groups):
                at = (u * groups + lo) * width
                out_ref[lo * high + step * per + u] = result[at : at + width].astype(BF16)


def triangle_kernel(side, groups, incoming, got_ref, send_ref):
    parts, _, rows, _ = got_ref.shape
    width = LANES // groups
    mine = rows // SUB
    turned = []
    for which in range(2):
        per_row = []
        for r in range(side):
            blocks = [got_ref[r * side + c, which].astype(F32) for c in range(side)]
            per_row.append(swap_groups(blocks, width))
        turned.append(per_row)
    sums = []
    for h in range(mine):
        span = slice(h * SUB, (h + 1) * SUB)
        left = jnp.concatenate([turned[0][r][lo][span] for lo in range(groups) for r in range(side)], axis=0).astype(BF16)
        if incoming:
            right = jnp.concatenate([turned[1][r][lo][span] for lo in range(groups) for r in range(side)], axis=0).astype(BF16)
            total = lax.dot_general(left, right, (((0,), (0,)), ((), ())), preferred_element_type=F32)
            pick = lambda r, lo: (r * groups + lo) * SUB
        else:
            right = jnp.concatenate([turned[1][r][lo][span] for r in range(side) for lo in range(groups)], axis=0).astype(BF16)
            total = lax.dot_general(left, right, (((1,), (1,)), ((), ())), preferred_element_type=F32)
            pick = lambda r, lo: (lo * side + r) * SUB
        sums.append([[total[pick(r, lo) : pick(r, lo) + SUB] for lo in range(groups)] for r in range(side)])
    for r in range(side):
        blocks = [jnp.concatenate([sums[h][r][lo] for h in range(mine)], axis=0) for lo in range(groups)]
        for c, block in enumerate(swap_groups(blocks, width)):
            send_ref[r * side + c] = block.astype(BF16)


def channel_split(side, *args):
    (x, mask, out_left_w, out_right_w, out_gate_w, out_final_w, in_left_w, in_right_w, in_gate_w, in_final_w,
     trans_in_w, trans_out_w) = args
    axes = ("row", "col")
    rows, width, channels = x.shape
    hidden = out_final_w.shape[0]
    groups = LANES // width
    high = rows // groups
    parts = side * side
    tokens = rows * width
    block = hidden // parts * high
    per = high
    shape = jax.ShapeDtypeStruct
    send = shape((parts, 2, block, LANES), BF16)
    back = shape((parts, block, LANES), BF16)
    gate = shape((channels, tokens), F32)
    base = shape((channels, tokens), BF16)
    lane_scr = pltpu.VMEM((high, LANES), F32)
    scr = pltpu.VMEM((2, hidden * high, LANES), F32)
    tri_scr = pltpu.VMEM((hidden * high, LANES), F32)

    def exchange(values):
        return lax.all_to_all(values, axes, split_axis=0, concat_axis=0, tiled=True)

    def triangle(got, incoming, name):
        return pl.pallas_call(functools.partial(triangle_kernel, side, groups, incoming), out_shape=back, name=name, compiler_params=PARAMS)(got)

    first = (x, mask, out_left_w, out_right_w, out_gate_w)
    sent, gate_out, base_out = pl.pallas_call(
        functools.partial(open_kernel, per, groups), out_shape=(send, gate, base), name="open", compiler_params=pltpu.CompilerParams(vmem_limit_bytes=60 * 1024 * 1024),
        in_specs=[pl.BlockSpec(memory_space=pltpu.HBM)] * len(first),
        scratch_shapes=[lane_scr, scr] + [pltpu.VMEM(a.shape, a.dtype) for a in first] + [pltpu.SemaphoreType.DMA((len(first),))],
    )(*first)
    returned = exchange(triangle(exchange(sent), False, "outgoing"))
    sent, gate_in, base_in = pl.pallas_call(
        functools.partial(middle_kernel, per, groups), out_shape=(send, gate, base),
        scratch_shapes=[lane_scr, scr, tri_scr], name="middle", compiler_params=PARAMS,
    )(returned, gate_out, base_out, out_final_w, mask, in_left_w, in_right_w, in_gate_w)
    returned = exchange(triangle(exchange(sent), True, "incoming"))
    return pl.pallas_call(
        functools.partial(close_kernel, per, groups), out_shape=shape(x.shape, BF16), scratch_shapes=[tri_scr], name="close", compiler_params=PARAMS
    )(returned, gate_in, base_in, in_final_w, trans_in_w, trans_out_w)


def layer_norm(values):
    average = jnp.mean(values, axis=-1, keepdims=True)
    centered = values - average
    spread = jnp.mean(centered * centered, axis=-1, keepdims=True)
    return centered * lax.rsqrt(spread + epsilon)


def gated(normed, weight, mask_vals):
    projected = jnp.dot(normed, weight, preferred_element_type=F32)
    half_width = weight.shape[1] // 2
    result = jax.nn.sigmoid(projected[..., :half_width]) * projected[..., half_width:]
    result = result * mask_vals[..., None]
    return result.astype(BF16)


def finish_plain(pair_repr, normed, triangle, gate_w, final_w):
    gate_vals = jax.nn.sigmoid(jnp.dot(normed, gate_w, preferred_element_type=F32))
    tri_norm = layer_norm(triangle).astype(BF16)
    update = jnp.dot(tri_norm, final_w, preferred_element_type=F32)
    return (pair_repr.astype(F32) + gate_vals * update).astype(BF16)


def gathers(pair_repr, pair_mask, out_left_w, out_right_w, out_gate_w, out_final_w, in_left_w, in_right_w, in_gate_w,
            in_final_w, trans_in_w, trans_out_w):
    mask_vals = pair_mask.astype(F32)
    normed_out = layer_norm(pair_repr.astype(F32)).astype(BF16)
    outbound = gated(normed_out, out_right_w, mask_vals)
    turned_right = lax.all_to_all(
        lax.all_to_all(outbound, "row", split_axis=0, concat_axis=0, tiled=True),
        "col", split_axis=0, concat_axis=1, tiled=True,
    )
    left_tile = gated(normed_out, out_left_w, mask_vals)
    gathered = lax.all_gather(left_tile, "col", axis=1, tiled=True)
    triangle = jnp.einsum(
        "ikh,jkh->ijh", gathered, lax.all_gather(turned_right, "row", axis=0, tiled=True), preferred_element_type=F32
    )
    middle = finish_plain(pair_repr, normed_out, triangle, out_gate_w, out_final_w)
    normed_in = layer_norm(middle.astype(F32)).astype(BF16)
    outbound_left = gated(normed_in, in_left_w, mask_vals)
    turned_left = lax.all_to_all(
        lax.all_to_all(outbound_left, "col", split_axis=1, concat_axis=1, tiled=True),
        "row", split_axis=1, concat_axis=0, tiled=True,
    )
    right_tile = gated(normed_in, in_right_w, mask_vals)
    column_panel = lax.all_gather(right_tile, "row", axis=0, tiled=True)
    triangle_in = jnp.einsum(
        "kih,kjh->ijh", lax.all_gather(turned_left, "col", axis=1, tiled=True), column_panel, preferred_element_type=F32
    )
    after_in = finish_plain(middle, normed_in, triangle_in, in_gate_w, in_final_w)
    normed_mix = layer_norm(after_in.astype(F32)).astype(BF16)
    projected = jnp.dot(normed_mix, trans_in_w, preferred_element_type=F32)
    half_width = trans_in_w.shape[1] // 2
    hidden = (jax.nn.silu(projected[..., :half_width]) * projected[..., half_width:]).astype(BF16)
    result = after_in.astype(F32) + jnp.dot(hidden, trans_out_w, preferred_element_type=F32)
    return result.astype(BF16)


def shards(row_size, col_size, *args):
    rows, width, channels = args[0].shape
    hidden = args[5].shape[0]
    fits = (
        row_size == col_size
        and rows == width
        and row_size * rows == LANES
        and rows % (LANES // width) == 0
        and rows // (LANES // width) == SUB
        and hidden % (row_size * col_size) == 0
        and channels == LANES
        and hidden == LANES
    )
    if fits:
        return channel_split(row_size, *args)
    return gathers(*args)


def solution(mesh):
    tile = P(("crop", "row"), "col")
    in_specs = (P(("crop", "row"), "col", None), tile) + (P(),) * 10
    out_specs = P(("crop", "row"), "col", None)
    body = functools.partial(shards, mesh.shape["row"], mesh.shape["col"])
    return jax.shard_map(body, mesh=mesh, in_specs=in_specs, out_specs=out_specs, check_vma=False)
```

```python
import functools

import jax
import jax.numpy as jnp
from jax import lax
from jax.experimental import pallas as pl
from jax.experimental.pallas import tpu as pltpu
from jax.sharding import PartitionSpec as P

epsilon = 1e-05
LANES = 128
SUB = 8
F32, BF16 = jnp.float32, jnp.bfloat16
OFFSET = 5000
PARAMS = pltpu.CompilerParams(vmem_limit_bytes=16 * 1024 * 1024)


def norm_rows(values):
    average = jnp.mean(values, axis=0, keepdims=True)
    centered = values - average
    spread = jnp.mean(centered * centered, axis=0, keepdims=True)
    return (centered * lax.rsqrt(spread + epsilon)).astype(BF16)


def sigmoid(values):
    return 0.5 * jnp.tanh(0.5 * values) + 0.5


def dot(a, b):
    return jnp.dot(a, b, preferred_element_type=F32)


def swap_groups(values, width):
    values = list(values)
    count = len(values)
    group = lax.broadcasted_iota(jnp.int32, values[0].shape, 1) // width
    bit = count // 2
    while bit:
        low = (group & bit) == 0
        for at in range(count):
            if at & bit:
                continue
            one, two = values[at], values[at | bit]
            values[at] = jnp.where(low, one, pltpu.roll(two, bit * width, 1))
            values[at | bit] = jnp.where(low, pltpu.roll(one, LANES - bit * width, 1), two)
        bit //= 2
    return values


def lane_mask(mask_ref, lane_ref, groups):
    rows, width = mask_ref.shape
    count = rows // groups
    for lo in range(groups):
        lane_ref[:, lo * width : (lo + 1) * width] = mask_ref[lo * count : (lo + 1) * count, :].astype(F32)


def project(normed, step, per, left_w, right_w, gate_w, lane_ref, scr_ref, gate_ref):
    half = left_w.shape[0] // 2
    high = lane_ref.shape[0]
    for side, weight in enumerate((left_w, right_w)):
        both = dot(weight, normed)
        value = sigmoid(both[:half]) * both[half:]
        for u in range(per):
            hi = step * per + u
            piece = value[:, u * LANES : (u + 1) * LANES] * lane_ref[hi : hi + 1, :]
            scr_ref[side, pl.ds(hi, half, stride=high), :] = piece
    if gate_ref is not None:
        gate_ref[:, step * per * LANES : (step + 1) * per * LANES] = sigmoid(dot(gate_w, normed))


def flush(scr_ref, send_ref):
    parts = send_ref.shape[0]
    for side in range(2):
        send_ref[:, side] = scr_ref[side].reshape(parts, -1, LANES).astype(BF16)


def finish(step, per, tri_ref, gate_ref, base_ref, final_w):
    high = tri_ref.shape[0] // final_w.shape[1]
    rows = final_w.shape[1]
    triangle = jnp.concatenate(
        [tri_ref[pl.ds(step * per + u, rows, stride=high), :] for u in range(per)], axis=1
    )
    update = dot(final_w, norm_rows(triangle))
    span = slice(step * per * LANES, (step + 1) * per * LANES)
    return base_ref[:, span].astype(F32) + gate_ref[:, span] * update


def open_kernel(per, groups, *refs):
    count = 4
    far, refs = refs[:count], refs[count:]
    send_ref, lane_ref, scr_ref, *near, sems = refs
    copies = [pltpu.make_async_copy(a, b, sems.at[at]) for at, (a, b) in enumerate(zip(far, near))]
    for copy in copies:
        copy.start()
    x_ref, mask_ref, lw_ref, rw_ref = near
    rows, width, channels = x_ref.shape
    high = rows // groups

    @pl.when(lax.axis_index("crop") == 0)
    def _():
        pl.delay(OFFSET)

    for copy in copies:
        copy.wait()
    lane_mask(mask_ref, lane_ref, groups)
    left_w, right_w = lw_ref[...].T, rw_ref[...].T
    for step in range(high // per):
        tokens = [x_ref[lo * high + step * per + u] for u in range(per) for lo in range(groups)]
        values = jnp.concatenate([t.astype(F32) for t in tokens], axis=0).T
        project(norm_rows(values), step, per, left_w, right_w, None, lane_ref, scr_ref, None)
    flush(scr_ref, send_ref)


def gate_kernel(groups, x_ref, gw_ref, gate_ref, base_ref):
    high = x_ref.shape[0] // groups
    tokens = [x_ref[lo * high + u] for u in range(high) for lo in range(groups)]
    values = jnp.concatenate([t.astype(F32) for t in tokens], axis=0).T
    base_ref[...] = values.astype(BF16)
    gate_ref[...] = sigmoid(dot(gw_ref[...].T, norm_rows(values)))


def middle_kernel(per, groups, back_ref, gate0_ref, base0_ref, fw_ref, mask_ref, lw_ref, rw_ref, gw_ref,
                  send_ref, gate_ref, base_ref, lane_ref, scr_ref, tri_ref):
    lane_mask(mask_ref, lane_ref, groups)
    tri_ref[...] = back_ref[...].reshape(tri_ref.shape).astype(F32)
    final_w = fw_ref[...].T
    left_w, right_w, gate_w = lw_ref[...].T, rw_ref[...].T, gw_ref[...].T
    for step in range(lane_ref.shape[0] // per):
        middle = finish(step, per, tri_ref, gate0_ref, base0_ref, final_w).astype(BF16)
        base_ref[:, step * per * LANES : (step + 1) * per * LANES] = middle
        project(norm_rows(middle.astype(F32)), step, per, left_w, right_w, gate_w, lane_ref, scr_ref, gate_ref)
    flush(scr_ref, send_ref)


def close_kernel(per, groups, back_ref, gate_ref, base_ref, fw_ref, inw_ref, outw_ref, out_ref, tri_ref):
    rows, width, channels = out_ref.shape
    high = rows // groups
    tri_ref[...] = back_ref[...].reshape(tri_ref.shape).astype(F32)
    final_w, in_w, out_w = fw_ref[...].T, inw_ref[...].T, outw_ref[...].T
    half = in_w.shape[0] // 2
    for step in range(high // per):
        after = finish(step, per, tri_ref, gate_ref, base_ref, final_w).astype(BF16).astype(F32)
        both = dot(in_w, norm_rows(after))
        swish = both[:half]
        hidden = (swish * sigmoid(swish) * both[half:]).astype(BF16)
        result = (after + dot(out_w, hidden)).T
        for u in range(per):
            for lo in range(groups):
                at = (u * groups + lo) * width
                out_ref[lo * high + step * per + u] = result[at : at + width].astype(BF16)


def triangle_kernel(side, groups, incoming, got_ref, send_ref):
    parts, _, rows, _ = got_ref.shape
    width = LANES // groups
    mine = rows // SUB
    turned = []
    for which in range(2):
        per_row = []
        for r in range(side):
            blocks = [got_ref[r * side + c, which] for c in range(side)]
            per_row.append(swap_groups(blocks, width))
        turned.append(per_row)
    sums = []
    for h in range(mine):
        span = slice(h * SUB, (h + 1) * SUB)
        left = jnp.concatenate([turned[0][r][lo][span] for lo in range(groups) for r in range(side)], axis=0)
        if incoming:
            right = jnp.concatenate([turned[1][r][lo][span] for lo in range(groups) for r in range(side)], axis=0)
            total = lax.dot_general(left, right, (((0,), (0,)), ((), ())), preferred_element_type=F32)
            pick = lambda r, lo: (r * groups + lo) * SUB
        else:
            right = jnp.concatenate([turned[1][r][lo][span] for r in range(side) for lo in range(groups)], axis=0)
            total = lax.dot_general(left, right, (((1,), (1,)), ((), ())), preferred_element_type=F32)
            pick = lambda r, lo: (lo * side + r) * SUB
        sums.append([[total[pick(r, lo) : pick(r, lo) + SUB] for lo in range(groups)] for r in range(side)])
    for r in range(side):
        blocks = [jnp.concatenate([sums[h][r][lo] for h in range(mine)], axis=0).astype(BF16) for lo in range(groups)]
        for c, block in enumerate(swap_groups(blocks, width)):
            send_ref[r * side + c] = block


def channel_split(side, *args):
    (x, mask, out_left_w, out_right_w, out_gate_w, out_final_w, in_left_w, in_right_w, in_gate_w, in_final_w,
     trans_in_w, trans_out_w) = args
    axes = ("row", "col")
    rows, width, channels = x.shape
    hidden = out_final_w.shape[0]
    groups = LANES // width
    high = rows // groups
    parts = side * side
    tokens = rows * width
    block = hidden // parts * high
    per = high
    shape = jax.ShapeDtypeStruct
    send = shape((parts, 2, block, LANES), BF16)
    back = shape((parts, block, LANES), BF16)
    gate = shape((channels, tokens), F32)
    base = shape((channels, tokens), BF16)
    lane_scr = pltpu.VMEM((high, LANES), F32)
    scr = pltpu.VMEM((2, hidden * high, LANES), F32)
    tri_scr = pltpu.VMEM((hidden * high, LANES), F32)

    def exchange(values):
        return lax.all_to_all(values, axes, split_axis=0, concat_axis=0, tiled=True)

    def triangle(got, incoming, name):
        return pl.pallas_call(functools.partial(triangle_kernel, side, groups, incoming), out_shape=back, name=name, compiler_params=PARAMS)(got)

    first = (x, mask, out_left_w, out_right_w)
    sent = pl.pallas_call(
        functools.partial(open_kernel, per, groups), out_shape=send, name="open", compiler_params=pltpu.CompilerParams(vmem_limit_bytes=60 * 1024 * 1024),
        in_specs=[pl.BlockSpec(memory_space=pltpu.HBM)] * len(first),
        scratch_shapes=[lane_scr, scr] + [pltpu.VMEM(a.shape, a.dtype) for a in first] + [pltpu.SemaphoreType.DMA((len(first),))],
    )(*first)
    gate_out, base_out = pl.pallas_call(
        functools.partial(gate_kernel, groups), out_shape=(gate, base), name="gate", compiler_params=PARAMS,
        cost_estimate=pl.CostEstimate(flops=1 << 34, bytes_accessed=1 << 20, transcendentals=0),
    )(x, out_gate_w)
    got, gate_out, base_out = lax.optimization_barrier((exchange(sent), gate_out, base_out))
    returned = exchange(triangle(got, False, "outgoing"))
    sent, gate_in, base_in = pl.pallas_call(
        functools.partial(middle_kernel, per, groups), out_shape=(send, gate, base),
        scratch_shapes=[lane_scr, scr, tri_scr], name="middle", compiler_params=PARAMS,
    )(returned, gate_out, base_out, out_final_w, mask, in_left_w, in_right_w, in_gate_w)
    returned = exchange(triangle(exchange(sent), True, "incoming"))
    return pl.pallas_call(
        functools.partial(close_kernel, per, groups), out_shape=shape(x.shape, BF16), scratch_shapes=[tri_scr], name="close", compiler_params=PARAMS
    )(returned, gate_in, base_in, in_final_w, trans_in_w, trans_out_w)


def layer_norm(values):
    average = jnp.mean(values, axis=-1, keepdims=True)
    centered = values - average
    spread = jnp.mean(centered * centered, axis=-1, keepdims=True)
    return centered * lax.rsqrt(spread + epsilon)


def gated(normed, weight, mask_vals):
    projected = jnp.dot(normed, weight, preferred_element_type=F32)
    half_width = weight.shape[1] // 2
    result = jax.nn.sigmoid(projected[..., :half_width]) * projected[..., half_width:]
    result = result * mask_vals[..., None]
    return result.astype(BF16)


def finish_plain(pair_repr, normed, triangle, gate_w, final_w):
    gate_vals = jax.nn.sigmoid(jnp.dot(normed, gate_w, preferred_element_type=F32))
    tri_norm = layer_norm(triangle).astype(BF16)
    update = jnp.dot(tri_norm, final_w, preferred_element_type=F32)
    return (pair_repr.astype(F32) + gate_vals * update).astype(BF16)


def gathers(pair_repr, pair_mask, out_left_w, out_right_w, out_gate_w, out_final_w, in_left_w, in_right_w, in_gate_w,
            in_final_w, trans_in_w, trans_out_w):
    mask_vals = pair_mask.astype(F32)
    normed_out = layer_norm(pair_repr.astype(F32)).astype(BF16)
    outbound = gated(normed_out, out_right_w, mask_vals)
    turned_right = lax.all_to_all(
        lax.all_to_all(outbound, "row", split_axis=0, concat_axis=0, tiled=True),
        "col", split_axis=0, concat_axis=1, tiled=True,
    )
    left_tile = gated(normed_out, out_left_w, mask_vals)
    gathered = lax.all_gather(left_tile, "col", axis=1, tiled=True)
    triangle = jnp.einsum(
        "ikh,jkh->ijh", gathered, lax.all_gather(turned_right, "row", axis=0, tiled=True), preferred_element_type=F32
    )
    middle = finish_plain(pair_repr, normed_out, triangle, out_gate_w, out_final_w)
    normed_in = layer_norm(middle.astype(F32)).astype(BF16)
    outbound_left = gated(normed_in, in_left_w, mask_vals)
    turned_left = lax.all_to_all(
        lax.all_to_all(outbound_left, "col", split_axis=1, concat_axis=1, tiled=True),
        "row", split_axis=1, concat_axis=0, tiled=True,
    )
    right_tile = gated(normed_in, in_right_w, mask_vals)
    column_panel = lax.all_gather(right_tile, "row", axis=0, tiled=True)
    triangle_in = jnp.einsum(
        "kih,kjh->ijh", lax.all_gather(turned_left, "col", axis=1, tiled=True), column_panel, preferred_element_type=F32
    )
    after_in = finish_plain(middle, normed_in, triangle_in, in_gate_w, in_final_w)
    normed_mix = layer_norm(after_in.astype(F32)).astype(BF16)
    projected = jnp.dot(normed_mix, trans_in_w, preferred_element_type=F32)
    half_width = trans_in_w.shape[1] // 2
    hidden = (jax.nn.silu(projected[..., :half_width]) * projected[..., half_width:]).astype(BF16)
    result = after_in.astype(F32) + jnp.dot(hidden, trans_out_w, preferred_element_type=F32)
    return result.astype(BF16)


def shards(row_size, col_size, *args):
    rows, width, channels = args[0].shape
    hidden = args[5].shape[0]
    fits = (
        row_size == col_size
        and rows == width
        and row_size * rows == LANES
        and rows % (LANES // width) == 0
        and rows // (LANES // width) == SUB
        and hidden % (row_size * col_size) == 0
        and channels == LANES
        and hidden == LANES
    )
    if fits:
        return channel_split(row_size, *args)
    return gathers(*args)


def solution(mesh):
    tile = P(("crop", "row"), "col")
    in_specs = (P(("crop", "row"), "col", None), tile) + (P(),) * 10
    out_specs = P(("crop", "row"), "col", None)
    body = functools.partial(shards, mesh.shape["row"], mesh.shape["col"])
    return jax.shard_map(body, mesh=mesh, in_specs=in_specs, out_specs=out_specs, check_vma=False)
```

```python
import functools

import jax
import jax.numpy as jnp
from jax import lax
from jax.experimental import pallas as pl
from jax.experimental.pallas import tpu as pltpu
from jax.sharding import PartitionSpec as P

epsilon = 1e-05
LANES = 128
SUB = 8
F32, BF16 = jnp.float32, jnp.bfloat16
OFFSET = 5000
PARAMS = pltpu.CompilerParams(vmem_limit_bytes=16 * 1024 * 1024)


def norm_rows(values):
    average = jnp.mean(values, axis=0, keepdims=True)
    centered = values - average
    spread = jnp.mean(centered * centered, axis=0, keepdims=True)
    return (centered * lax.rsqrt(spread + epsilon)).astype(BF16)


def sigmoid(values):
    return 0.5 * jnp.tanh(0.5 * values) + 0.5


def dot(a, b):
    return jnp.dot(a, b, preferred_element_type=F32)


def swap_groups(values, width):
    values = list(values)
    count = len(values)
    group = lax.broadcasted_iota(jnp.int32, values[0].shape, 1) // width
    bit = count // 2
    while bit:
        low = (group & bit) == 0
        for at in range(count):
            if at & bit:
                continue
            one, two = values[at], values[at | bit]
            values[at] = jnp.where(low, one, pltpu.roll(two, bit * width, 1))
            values[at | bit] = jnp.where(low, pltpu.roll(one, LANES - bit * width, 1), two)
        bit //= 2
    return values


def lane_mask(mask_ref, lane_ref, groups):
    rows, width = mask_ref.shape
    count = rows // groups
    for lo in range(groups):
        lane_ref[:, lo * width : (lo + 1) * width] = mask_ref[lo * count : (lo + 1) * count, :].astype(F32)


def project(normed, step, per, left_w, right_w, gate_w, lane_ref, scr_ref, gate_ref):
    half = left_w.shape[0] // 2
    high = lane_ref.shape[0]
    for side, weight in enumerate((left_w, right_w)):
        both = dot(weight, normed)
        value = sigmoid(both[:half]) * both[half:]
        for u in range(per):
            hi = step * per + u
            piece = value[:, u * LANES : (u + 1) * LANES] * lane_ref[hi : hi + 1, :]
            scr_ref[side, pl.ds(hi, half, stride=high), :] = piece
    if gate_ref is not None:
        gate_ref[:, step * per * LANES : (step + 1) * per * LANES] = sigmoid(dot(gate_w, normed))


def flush(scr_ref, send_ref):
    parts = send_ref.shape[0]
    for side in range(2):
        send_ref[:, side] = scr_ref[side].reshape(parts, -1, LANES).astype(BF16)


def finish(step, per, tri_ref, gate_ref, base_ref, final_w):
    high = tri_ref.shape[0] // final_w.shape[1]
    rows = final_w.shape[1]
    triangle = jnp.concatenate(
        [tri_ref[pl.ds(step * per + u, rows, stride=high), :] for u in range(per)], axis=1
    )
    update = dot(final_w, norm_rows(triangle))
    span = slice(step * per * LANES, (step + 1) * per * LANES)
    return base_ref[:, span].astype(F32) + gate_ref[:, span] * update


def open_kernel(per, groups, *refs):
    count = 4
    far, refs = refs[:count], refs[count:]
    send_ref, lane_ref, scr_ref, *near, sems = refs
    copies = [pltpu.make_async_copy(a, b, sems.at[at]) for at, (a, b) in enumerate(zip(far, near))]
    for copy in copies:
        copy.start()
    x_ref, mask_ref, lw_ref, rw_ref = near
    rows, width, channels = x_ref.shape
    high = rows // groups

    @pl.when(lax.axis_index("crop") == 0)
    def _():
        pl.delay(OFFSET)

    for copy in copies:
        copy.wait()
    lane_mask(mask_ref, lane_ref, groups)
    left_w, right_w = lw_ref[...].T, rw_ref[...].T
    for step in range(high // per):
        tokens = [x_ref[lo * high + step * per + u] for u in range(per) for lo in range(groups)]
        values = jnp.concatenate([t.astype(F32) for t in tokens], axis=0).T
        project(norm_rows(values), step, per, left_w, right_w, None, lane_ref, scr_ref, None)
    flush(scr_ref, send_ref)


def gate_kernel(groups, x_ref, gw_ref, gate_ref, base_ref):
    high = x_ref.shape[0] // groups
    tokens = [x_ref[lo * high + u] for u in range(high) for lo in range(groups)]
    values = jnp.concatenate([t.astype(F32) for t in tokens], axis=0).T
    base_ref[...] = values.astype(BF16)
    gate_ref[...] = sigmoid(dot(gw_ref[...].T, norm_rows(values)))


def middle_kernel(per, groups, back_ref, gate0_ref, base0_ref, fw_ref, mask_ref, lw_ref, rw_ref, gw_ref,
                  send_ref, gate_ref, base_ref, lane_ref, scr_ref, tri_ref):
    lane_mask(mask_ref, lane_ref, groups)
    tri_ref[...] = back_ref[...].reshape(tri_ref.shape).astype(F32)
    final_w = fw_ref[...].T
    left_w, right_w, gate_w = lw_ref[...].T, rw_ref[...].T, gw_ref[...].T
    for step in range(lane_ref.shape[0] // per):
        middle = finish(step, per, tri_ref, gate0_ref, base0_ref, final_w).astype(BF16)
        base_ref[:, step * per * LANES : (step + 1) * per * LANES] = middle
        project(norm_rows(middle.astype(F32)), step, per, left_w, right_w, gate_w, lane_ref, scr_ref, gate_ref)
    flush(scr_ref, send_ref)


def close_kernel(per, groups, back_ref, gate_ref, base_ref, fw_ref, inw_ref, outw_ref, out_ref, tri_ref):
    rows, width, channels = out_ref.shape
    high = rows // groups
    tri_ref[...] = back_ref[...].reshape(tri_ref.shape).astype(F32)
    final_w, in_w, out_w = fw_ref[...].T, inw_ref[...].T, outw_ref[...].T
    half = in_w.shape[0] // 2
    for step in range(high // per):
        after = finish(step, per, tri_ref, gate_ref, base_ref, final_w).astype(BF16).astype(F32)
        both = dot(in_w, norm_rows(after))
        swish = both[:half]
        hidden = (swish * sigmoid(swish) * both[half:]).astype(BF16)
        result = (after + dot(out_w, hidden)).T
        for u in range(per):
            for lo in range(groups):
                at = (u * groups + lo) * width
                out_ref[lo * high + step * per + u] = result[at : at + width].astype(BF16)


def triangle_kernel(side, groups, incoming, got_ref, send_ref):
    parts, _, rows, _ = got_ref.shape
    width = LANES // groups
    mine = rows // SUB
    turned = []
    for which in range(2):
        per_row = []
        for r in range(side):
            blocks = [got_ref[c * side + r, which] for c in range(side)]
            per_row.append(swap_groups(blocks, width))
        turned.append(per_row)
    sums = []
    for h in range(mine):
        span = slice(h * SUB, (h + 1) * SUB)
        left = jnp.concatenate([turned[0][r][lo][span] for lo in range(groups) for r in range(side)], axis=0)
        if incoming:
            right = jnp.concatenate([turned[1][r][lo][span] for lo in range(groups) for r in range(side)], axis=0)
            total = lax.dot_general(left, right, (((0,), (0,)), ((), ())), preferred_element_type=F32)
            pick = lambda r, lo: (r * groups + lo) * SUB
        else:
            right = jnp.concatenate([turned[1][r][lo][span] for r in range(side) for lo in range(groups)], axis=0)
            total = lax.dot_general(left, right, (((1,), (1,)), ((), ())), preferred_element_type=F32)
            pick = lambda r, lo: (lo * side + r) * SUB
        sums.append([[total[pick(r, lo) : pick(r, lo) + SUB] for lo in range(groups)] for r in range(side)])
    for r in range(side):
        blocks = [jnp.concatenate([sums[h][r][lo] for h in range(mine)], axis=0).astype(BF16) for lo in range(groups)]
        for c, block in enumerate(swap_groups(blocks, width)):
            send_ref[c * side + r] = block


def channel_split(side, *args):
    (x, mask, out_left_w, out_right_w, out_gate_w, out_final_w, in_left_w, in_right_w, in_gate_w, in_final_w,
     trans_in_w, trans_out_w) = args
    axes = ("col", "row")
    rows, width, channels = x.shape
    hidden = out_final_w.shape[0]
    groups = LANES // width
    high = rows // groups
    parts = side * side
    tokens = rows * width
    block = hidden // parts * high
    per = high
    shape = jax.ShapeDtypeStruct
    send = shape((parts, 2, block, LANES), BF16)
    back = shape((parts, block, LANES), BF16)
    gate = shape((channels, tokens), F32)
    base = shape((channels, tokens), BF16)
    lane_scr = pltpu.VMEM((high, LANES), F32)
    scr = pltpu.VMEM((2, hidden * high, LANES), F32)
    tri_scr = pltpu.VMEM((hidden * high, LANES), F32)

    def exchange(values):
        return lax.all_to_all(values, axes, split_axis=0, concat_axis=0, tiled=True)

    def triangle(got, incoming, name):
        return pl.pallas_call(functools.partial(triangle_kernel, side, groups, incoming), out_shape=back, name=name, compiler_params=PARAMS)(got)

    first = (x, mask, out_left_w, out_right_w)
    sent = pl.pallas_call(
        functools.partial(open_kernel, per, groups), out_shape=send, name="open", compiler_params=pltpu.CompilerParams(vmem_limit_bytes=60 * 1024 * 1024),
        in_specs=[pl.BlockSpec(memory_space=pltpu.HBM)] * len(first),
        scratch_shapes=[lane_scr, scr] + [pltpu.VMEM(a.shape, a.dtype) for a in first] + [pltpu.SemaphoreType.DMA((len(first),))],
    )(*first)
    gate_out, base_out = pl.pallas_call(
        functools.partial(gate_kernel, groups), out_shape=(gate, base), name="gate", compiler_params=PARAMS,
        cost_estimate=pl.CostEstimate(flops=1 << 34, bytes_accessed=1 << 20, transcendentals=0),
    )(x, out_gate_w)
    got, gate_out, base_out = lax.optimization_barrier((exchange(sent), gate_out, base_out))
    returned = exchange(triangle(got, False, "outgoing"))
    sent, gate_in, base_in = pl.pallas_call(
        functools.partial(middle_kernel, per, groups), out_shape=(send, gate, base),
        scratch_shapes=[lane_scr, scr, tri_scr], name="middle", compiler_params=PARAMS,
    )(returned, gate_out, base_out, out_final_w, mask, in_left_w, in_right_w, in_gate_w)
    returned = exchange(triangle(exchange(sent), True, "incoming"))
    return pl.pallas_call(
        functools.partial(close_kernel, per, groups), out_shape=shape(x.shape, BF16), scratch_shapes=[tri_scr], name="close", compiler_params=PARAMS
    )(returned, gate_in, base_in, in_final_w, trans_in_w, trans_out_w)


def layer_norm(values):
    average = jnp.mean(values, axis=-1, keepdims=True)
    centered = values - average
    spread = jnp.mean(centered * centered, axis=-1, keepdims=True)
    return centered * lax.rsqrt(spread + epsilon)


def gated(normed, weight, mask_vals):
    projected = jnp.dot(normed, weight, preferred_element_type=F32)
    half_width = weight.shape[1] // 2
    result = jax.nn.sigmoid(projected[..., :half_width]) * projected[..., half_width:]
    result = result * mask_vals[..., None]
    return result.astype(BF16)


def finish_plain(pair_repr, normed, triangle, gate_w, final_w):
    gate_vals = jax.nn.sigmoid(jnp.dot(normed, gate_w, preferred_element_type=F32))
    tri_norm = layer_norm(triangle).astype(BF16)
    update = jnp.dot(tri_norm, final_w, preferred_element_type=F32)
    return (pair_repr.astype(F32) + gate_vals * update).astype(BF16)


def gathers(pair_repr, pair_mask, out_left_w, out_right_w, out_gate_w, out_final_w, in_left_w, in_right_w, in_gate_w,
            in_final_w, trans_in_w, trans_out_w):
    mask_vals = pair_mask.astype(F32)
    normed_out = layer_norm(pair_repr.astype(F32)).astype(BF16)
    outbound = gated(normed_out, out_right_w, mask_vals)
    turned_right = lax.all_to_all(
        lax.all_to_all(outbound, "row", split_axis=0, concat_axis=0, tiled=True),
        "col", split_axis=0, concat_axis=1, tiled=True,
    )
    left_tile = gated(normed_out, out_left_w, mask_vals)
    gathered = lax.all_gather(left_tile, "col", axis=1, tiled=True)
    triangle = jnp.einsum(
        "ikh,jkh->ijh", gathered, lax.all_gather(turned_right, "row", axis=0, tiled=True), preferred_element_type=F32
    )
    middle = finish_plain(pair_repr, normed_out, triangle, out_gate_w, out_final_w)
    normed_in = layer_norm(middle.astype(F32)).astype(BF16)
    outbound_left = gated(normed_in, in_left_w, mask_vals)
    turned_left = lax.all_to_all(
        lax.all_to_all(outbound_left, "col", split_axis=1, concat_axis=1, tiled=True),
        "row", split_axis=1, concat_axis=0, tiled=True,
    )
    right_tile = gated(normed_in, in_right_w, mask_vals)
    column_panel = lax.all_gather(right_tile, "row", axis=0, tiled=True)
    triangle_in = jnp.einsum(
        "kih,kjh->ijh", lax.all_gather(turned_left, "col", axis=1, tiled=True), column_panel, preferred_element_type=F32
    )
    after_in = finish_plain(middle, normed_in, triangle_in, in_gate_w, in_final_w)
    normed_mix = layer_norm(after_in.astype(F32)).astype(BF16)
    projected = jnp.dot(normed_mix, trans_in_w, preferred_element_type=F32)
    half_width = trans_in_w.shape[1] // 2
    hidden = (jax.nn.silu(projected[..., :half_width]) * projected[..., half_width:]).astype(BF16)
    result = after_in.astype(F32) + jnp.dot(hidden, trans_out_w, preferred_element_type=F32)
    return result.astype(BF16)


def shards(row_size, col_size, *args):
    rows, width, channels = args[0].shape
    hidden = args[5].shape[0]
    fits = (
        row_size == col_size
        and rows == width
        and row_size * rows == LANES
        and rows % (LANES // width) == 0
        and rows // (LANES // width) == SUB
        and hidden % (row_size * col_size) == 0
        and channels == LANES
        and hidden == LANES
    )
    if fits:
        return channel_split(row_size, *args)
    return gathers(*args)


def solution(mesh):
    tile = P(("crop", "row"), "col")
    in_specs = (P(("crop", "row"), "col", None), tile) + (P(),) * 10
    out_specs = P(("crop", "row"), "col", None)
    body = functools.partial(shards, mesh.shape["row"], mesh.shape["col"])
    return jax.shard_map(body, mesh=mesh, in_specs=in_specs, out_specs=out_specs, check_vma=False)
```
